256 devices in a mesh: track: 64 (over z, y_hi, x), lane: 4 (over y_lo, core).
Axes of the slice: x: 4, y: 4 (y_hi: 2, y_lo: 2; y = y_hi * 2 + y_lo), z: 8, core: 2. Of those that a mesh axis runs over, the one named last changes fastest.
Arguments:
- signal: float32 [64, 4, 4096, 512], P('track', 'lane'), may hold values from -8 to 8, as said below
- tap_gain: float32 [3, 512], replicated, may hold values from 0.3 to 1.2
Outputs:
- filtered: float32 [64, 4, 4096, 512], P('track', 'lane')
The draws below stay inside these ranges and needn't reach their ends.
Inputs may be any that keep to these rules, and one draw needn't show every extreme that they name: signal holds numbers from -8 to 8.
All inputs are finite; a program needn't handle non-finite values.
Results may differ from the reference program's by a relative error of at most 0.0003.
Values sent between devices are 32-bit elements.
A program may use at most 64 MiB of HBM per device.

```python
import jax
import jax.numpy as jnp

STEPS_DEV = 4096
CHANNELS = 512
SEGMENTS = 64
RECORDS = 4


def draw_signal(key, part):
    keys = jax.random.split(key, 2)
    loud = jnp.exp(jax.random.uniform(keys[0], (SEGMENTS, RECORDS, 1, CHANNELS), jnp.float32, -1.2, 1.2))
    noise = jax.random.normal(keys[1], (SEGMENTS, RECORDS, STEPS_DEV, CHANNELS), jnp.float32)
    return jnp.clip(loud * noise, -8.0, 8.0)


def setup_inputs(seed: int = 0) -> dict:
    seeds = jax.random.split(jax.random.key(seed), 3)
    signal = draw_signal(jax.random.fold_in(seeds[2], 71), 0)
    tap_gain = jnp.clip(jax.random.uniform(seeds[1], (3, CHANNELS), jnp.float32, 0.3, 1.2), 0.3, 1.2)
    return {"signal": signal, "tap_gain": tap_gain}


def reference(signal, tap_gain):
    wide_in = signal.astype(jnp.float32)
    mixed = tap_gain[0] * wide_in + tap_gain[1] * jnp.roll(wide_in, 1, axis=0) + tap_gain[2] * jnp.roll(wide_in, 2, axis=0)
    filtered = jnp.tanh(mixed).astype(jnp.float32)
    return filtered
```

```python
import functools

import jax
import jax.numpy as jnp
from jax import lax
from jax.experimental import pallas as pl
from jax.experimental.pallas import tpu as pltpu
from jax.sharding import PartitionSpec as P

CHUNKS = 64
LAG = 4
LOADS = 4


def kernel(n, signal, gain, out, own, near, far, part, load_sem, near_send, near_recv, far_send, far_recv):
    steps = own.shape[0]
    rows = steps // CHUNKS
    t = lax.axis_index("track")
    x, y = t % 4, (t // 4) % 2
    odd = x % 2
    last = (x // 3) * y
    relay = (x // 2) * (1 - odd) * y
    first = odd * (1 - x // 3) * (1 - y)

    def piece(k):
        return pl.ds(pl.multiple_of(k * rows, rows), rows)

    def device(offset):
        return {"track": (t + offset + n) % n}

    def near_copy(src, k):
        return pltpu.make_async_remote_copy(
            src_ref=src.at[piece(k)],
            dst_ref=near.at[piece(k)],
            send_sem=near_send.at[k],
            recv_sem=near_recv.at[k],
            device_id=device(1),
            device_id_type=pl.DeviceIdType.MESH,
        )

    def far_copy(src, k, offset):
        return pltpu.make_async_remote_copy(
            src_ref=src.at[piece(k)],
            dst_ref=far.at[piece(k)],
            send_sem=far_send.at[k],
            recv_sem=far_recv.at[k],
            device_id=device(offset),
            device_id_type=pl.DeviceIdType.MESH,
        )

    loads = []
    for i in range(LOADS):
        block = pl.ds(i * (steps // LOADS), steps // LOADS)
        loads.append(pltpu.make_async_copy(signal.at[0, 0, block], own.at[block], load_sem.at[i]))
        loads[-1].start()

    barrier = pltpu.get_barrier_semaphore()

    def greet(offset):
        pl.semaphore_signal(barrier, inc=1, device_id=device(offset), device_id_type=pl.DeviceIdType.MESH)

    greet(-1)

    @pl.when(odd == 1)
    def _():
        greet(-2 - first)

    @pl.when(relay == 1)
    def _():
        greet(1)

    for load in loads:
        load.wait()
    pl.semaphore_wait(barrier, 1 + odd + relay)

    g0, g1, g2 = gain[0:1], gain[1:2], gain[2:3]

    @pl.when(odd == 1)
    def _():
        far_to = 2 - 3 * last

        def send(k, _):
            far_copy(own, k, far_to).start()
            return 0

        lax.fori_loop(0, CHUNKS, send, 0)

        def finish(k):
            far_copy(own, k, far_to).wait_recv()
            at = piece(k)
            out[at] = jnp.tanh(out[at] + g2 * far[at])

        def step(k, _):
            near_copy(part, k).wait_recv()
            at = piece(k)
            mine, before = own[at], near[at]
            part[at] = g1 * mine + g2 * before
            out[at] = g0 * mine + g1 * before
            near_copy(part, k).start()

            @pl.when(k >= LAG)
            def _():
                finish(k - LAG)

            return 0

        lax.fori_loop(0, CHUNKS, step, 0)

        def tail(k, _):
            finish(k)
            return 0

        lax.fori_loop(CHUNKS - LAG, CHUNKS, tail, 0)

        def drain(k, _):
            far_copy(own, k, far_to).wait_send()
            near_copy(part, k).wait_send()
            return 0

        lax.fori_loop(0, CHUNKS, drain, 0)

    @pl.when(odd == 0)
    def _():
        def send(k, _):
            near_copy(own, k).start()
            return 0

        lax.fori_loop(0, CHUNKS, send, 0)

        def step(k, _):
            @pl.when(relay == 1)
            def _():
                far_copy(far, k, 3).wait_recv()
                far_copy(far, k, 3).start()

            near_copy(own, k).wait_recv()
            at = piece(k)
            out[at] = jnp.tanh(g0 * own[at] + near[at])
            return 0

        lax.fori_loop(0, CHUNKS, step, 0)

        def drain(k, _):
            near_copy(own, k).wait_send()

            @pl.when(relay == 1)
            def _():
                far_copy(far, k, 3).wait_send()

            return 0

        lax.fori_loop(0, CHUNKS, drain, 0)


def local(n, signal, tap_gain):
    steps, channels = signal.shape[2:]
    whole = pltpu.VMEM((steps, channels), jnp.float32)
    sems = pltpu.SemaphoreType.DMA((CHUNKS,))
    out = pl.pallas_call(
        functools.partial(kernel, n),
        out_shape=pltpu.VMEM((steps, channels), jnp.float32),
        in_specs=[pl.BlockSpec(memory_space=pl.ANY), pl.BlockSpec(memory_space=pltpu.VMEM)],
        out_specs=pl.BlockSpec(memory_space=pltpu.VMEM),
        scratch_shapes=[whole] * 4 + [pltpu.SemaphoreType.DMA((LOADS,))] + [sems] * 4,
        compiler_params=pltpu.CompilerParams(
            collective_id=0, has_side_effects=True, vmem_limit_bytes=40 * 2**20
        ),
        name="echo",
    )(signal, tap_gain)
    return out.reshape(signal.shape)


def solution(mesh):
    in_specs = (P("track", "lane", None, None), P())
    out_specs = P("track", "lane", None, None)
    body = functools.partial(local, mesh.shape["track"])
    return jax.shard_map(body, mesh=mesh, in_specs=in_specs, out_specs=out_specs, check_vma=False)
```

```python
import functools

import jax
import jax.numpy as jnp
from jax import lax
from jax.experimental import pallas as pl
from jax.experimental.pallas import tpu as pltpu
from jax.sharding import PartitionSpec as P

BLOCK = 64
SHARES = (16, 16, 16, 8, 4, 2, 2)


def kernel(n, sizes, signal, gain, out, own, near, far, part, gains, gain_sem, load_sem, near_send, near_recv, far_send, far_recv):
    half = own.shape[0] // 2
    count = len(sizes)
    starts = [sum(sizes[:i]) for i in range(count)]
    t = lax.axis_index("track")
    odd = t % 2
    raw_half = odd
    sum_half = 1 - odd
    far_to = 3 - 4 * odd
    far_from = 1 - 4 * odd

    def device(offset):
        return {"track": (t + offset + n) % n}

    barrier = pltpu.get_barrier_semaphore()
    for source in (-1, far_from):
        pl.semaphore_signal(barrier, inc=1, device_id=device(source), device_id_type=pl.DeviceIdType.MESH)

    def rows(side, i):
        return pl.ds(pl.multiple_of(side * half + starts[i], BLOCK), sizes[i])

    def near_copy(src, src_rows, side, i):
        return pltpu.make_async_remote_copy(
            src_ref=src.at[src_rows],
            dst_ref=near.at[rows(side, i)],
            send_sem=near_send.at[side * count + i],
            recv_sem=near_recv.at[side * count + i],
            device_id=device(1),
            device_id_type=pl.DeviceIdType.MESH,
        )

    def near_raw(i):
        return near_copy(own, rows(raw_half, i), raw_half, i)

    def near_sum(i):
        return near_copy(part, pl.ds(starts[i], sizes[i]), sum_half, i)

    def far_copy(src, side, i):
        return pltpu.make_async_remote_copy(
            src_ref=src.at[rows(side, i)],
            dst_ref=far.at[rows(side, i)],
            send_sem=far_send.at[side * count + i],
            recv_sem=far_recv.at[side * count + i],
            device_id=device(far_to),
            device_id_type=pl.DeviceIdType.MESH,
        )

    def load(side, i):
        at = rows(side, i)
        return pltpu.make_async_copy(signal.at[0, 0, at], own.at[at], load_sem.at[side * count + i])

    for i in range(count):
        load(raw_half, i).start()
        load(sum_half, i).start()
    gain_load = pltpu.make_async_copy(gain, gains, gain_sem)
    gain_load.start()
    gain_load.wait()
    pl.semaphore_wait(barrier, 2)

    for i in range(count):
        load(raw_half, i).wait()
        near_raw(i).start()
        load(sum_half, i).wait()
        far_copy(own, sum_half, i).start()

    g0, g1, g2 = gains[0:1], gains[1:2], gains[2:3]

    def blocks(side, i, body):
        def step(j, _):
            offset = starts[i] + j * BLOCK
            body(pl.ds(pl.multiple_of(side * half + offset, BLOCK), BLOCK), pl.ds(pl.multiple_of(offset, BLOCK), BLOCK))
            return 0

        lax.fori_loop(0, sizes[i] // BLOCK, step, 0)

    def add_up(at, inner):
        mine, before = own[at], near[at]
        part[inner] = g1 * mine + g2 * before
        out[at] = g0 * mine + g1 * before

    def finish_raw(at, _):
        out[at] = jnp.tanh(g0 * own[at] + near[at])

    def finish_sum(at, _):
        out[at] = jnp.tanh(out[at] + g2 * far[at])

    for i in range(count):
        near_sum(i).wait_recv()
        blocks(sum_half, i, add_up)
        far_copy(far, raw_half, i).wait_recv()
        far_copy(far, raw_half, i).start()
        near_sum(i).start()

    for i in range(count):
        near_raw(i).wait_recv()
        blocks(raw_half, i, finish_raw)
        far_copy(far, sum_half, i).wait_recv()
        blocks(sum_half, i, finish_sum)

    for i in range(count):
        near_raw(i).wait_send()
        near_sum(i).wait_send()
        far_copy(own, sum_half, i).wait_send()
        far_copy(far, raw_half, i).wait_send()


def local(n, signal, tap_gain):
    steps, channels = signal.shape[2:]
    sizes = [steps // 2 * share // sum(SHARES) for share in SHARES]

    def buffer(rows):
        return pltpu.VMEM((rows, channels), jnp.float32)

    sems = pltpu.SemaphoreType.DMA((2 * len(sizes),))
    out = pl.pallas_call(
        functools.partial(kernel, n, sizes),
        out_shape=buffer(steps),
        in_specs=[pl.BlockSpec(memory_space=pl.ANY)] * 2,
        out_specs=pl.BlockSpec(memory_space=pltpu.VMEM),
        scratch_shapes=[buffer(steps)] * 3
        + [buffer(steps // 2), buffer(tap_gain.shape[0]), pltpu.SemaphoreType.DMA]
        + [sems] * 5,
        compiler_params=pltpu.CompilerParams(
            collective_id=0, has_side_effects=True, vmem_limit_bytes=52 * 2**20
        ),
        name="echo",
    )(signal, tap_gain)
    return out.reshape(signal.shape)


def solution(mesh):
    in_specs = (P("track", "lane", None, None), P())
    out_specs = P("track", "lane", None, None)
    body = functools.partial(local, mesh.shape["track"])
    return jax.shard_map(body, mesh=mesh, in_specs=in_specs, out_specs=out_specs, check_vma=False)
```

```python
import functools

import jax
import jax.numpy as jnp
from jax import lax
from jax.experimental import pallas as pl
from jax.experimental.pallas import tpu as pltpu
from jax.sharding import PartitionSpec as P

BLOCK = 64
SHARES = (16, 16, 16, 8, 2, 2, 2, 2)
DETOUR = 4


def kernel(n, sizes, signal, gain, out, own, near, far, part, gains, gain_sem, load_sem, near_send, near_recv, far_send, far_recv, aside, aside_send, aside_recv):
    half = own.shape[0] // 2
    count = len(sizes)
    starts = [sum(sizes[:i]) for i in range(count)]
    t = lax.axis_index("track")
    odd = t % 2
    raw_half = odd
    sum_half = 1 - odd
    far_to = 3 - 4 * odd
    far_from = 1 - 4 * odd

    ending = t // (n - 2)
    helper = (t // (n - 6)) * (1 - t // (n - 4))

    def device(offset):
        return {"track": (t + offset + n) % n}

    barrier = pltpu.get_barrier_semaphore()
    for source in (-1, far_from):
        pl.semaphore_signal(barrier, inc=1, device_id=device(source), device_id_type=pl.DeviceIdType.MESH)

    @pl.when(helper == 1)
    def _():
        pl.semaphore_signal(barrier, inc=1, device_id=device(4), device_id_type=pl.DeviceIdType.MESH)

    def rows(side, i):
        return pl.ds(pl.multiple_of(side * half + starts[i], BLOCK), sizes[i])

    def near_copy(src, src_rows, side, i):
        return pltpu.make_async_remote_copy(
            src_ref=src.at[src_rows],
            dst_ref=near.at[rows(side, i)],
            send_sem=near_send.at[side * count + i],
            recv_sem=near_recv.at[side * count + i],
            device_id=device(1),
            device_id_type=pl.DeviceIdType.MESH,
        )

    def near_raw(i):
        return near_copy(own, rows(raw_half, i), raw_half, i)

    def near_sum(i):
        return near_copy(part, pl.ds(starts[i], sizes[i]), sum_half, i)

    def far_copy(src, side, i):
        return pltpu.make_async_remote_copy(
            src_ref=src.at[rows(side, i)],
            dst_ref=far.at[rows(side, i)],
            send_sem=far_send.at[side * count + i],
            recv_sem=far_recv.at[side * count + i],
            device_id=device(far_to),
            device_id_type=pl.DeviceIdType.MESH,
        )

    def aside_copy(send_sem):
        return pltpu.make_async_remote_copy(
            src_ref=own.at[rows(1, DETOUR)],
            dst_ref=aside,
            send_sem=send_sem,
            recv_sem=aside_recv,
            device_id=device(-4),
            device_id_type=pl.DeviceIdType.MESH,
        )

    def back_copy(dst, recv_sem, offset):
        return pltpu.make_async_remote_copy(
            src_ref=aside,
            dst_ref=dst.at[rows(1, DETOUR)],
            send_sem=aside_send,
            recv_sem=recv_sem.at[count + DETOUR],
            device_id=device(offset),
            device_id_type=pl.DeviceIdType.MESH,
        )

    def start(copy, i, way):
        if i != DETOUR:
            copy.start()
            return

        @pl.when(way == 0)
        def _():
            copy.start()

    def load(side, i):
        at = rows(side, i)
        return pltpu.make_async_copy(signal.at[0, 0, at], own.at[at], load_sem.at[side * count + i])

    for i in range(count):
        load(raw_half, i).start()
        load(sum_half, i).start()
    gain_load = pltpu.make_async_copy(gain, gains, gain_sem)
    gain_load.start()
    pl.semaphore_wait(barrier, 2 + ending)

    for i in range(count):
        if i == 0:
            near_copy(signal.at[0, 0], rows(raw_half, i), raw_half, i).start()
            far_copy(signal.at[0, 0], sum_half, i).start()
            continue
        load(raw_half, i).wait()
        start(near_raw(i), i, ending * odd)
        load(sum_half, i).wait()
        start(far_copy(own, sum_half, i), i, ending * (1 - odd))

    @pl.when(ending * odd == 1)
    def _():
        aside_copy(near_send.at[count + DETOUR]).start()

    @pl.when(ending * (1 - odd) == 1)
    def _():
        aside_copy(far_send.at[count + DETOUR]).start()

    @pl.when(helper == 1)
    def _():
        aside_copy(aside_send).wait_recv()

    @pl.when(helper * odd == 1)
    def _():
        back_copy(near, near_recv, 5).start()

    @pl.when(helper * (1 - odd) == 1)
    def _():
        back_copy(far, far_recv, 7).start()

    gain_load.wait()
    load(raw_half, 0).wait()
    load(sum_half, 0).wait()
    g0, g1, g2 = gains[0:1], gains[1:2], gains[2:3]

    def blocks(side, i, body):
        def step(j, _):
            offset = starts[i] + j * BLOCK
            body(pl.ds(pl.multiple_of(side * half + offset, BLOCK), BLOCK), pl.ds(pl.multiple_of(offset, BLOCK), BLOCK))
            return 0

        lax.fori_loop(0, sizes[i] // BLOCK, step, 0)

    def add_up(at, inner):
        mine, before = own[at], near[at]
        part[inner] = g1 * mine + g2 * before
        out[at] = g0 * mine + g1 * before

    def finish_raw(at, _):
        out[at] = jnp.tanh(g0 * own[at] + near[at])

    def finish_sum(at, _):
        out[at] = jnp.tanh(out[at] + g2 * far[at])

    for i in range(count):
        near_sum(i).wait_recv()
        blocks(sum_half, i, add_up)
        far_copy(far, raw_half, i).wait_recv()
        far_copy(far, raw_half, i).start()
        near_sum(i).start()

    for i in range(count):
        near_raw(i).wait_recv()
        blocks(raw_half, i, finish_raw)
        far_copy(far, sum_half, i).wait_recv()
        blocks(sum_half, i, finish_sum)

    for i in range(count):
        near_raw(i).wait_send()
        near_sum(i).wait_send()
        far_copy(own, sum_half, i).wait_send()
        far_copy(far, raw_half, i).wait_send()

    @pl.when(helper == 1)
    def _():
        back_copy(far, far_recv, 7).wait_send()


def local(n, signal, tap_gain):
    steps, channels = signal.shape[2:]
    sizes = [steps // 2 * share // sum(SHARES) for share in SHARES]

    def buffer(rows):
        return pltpu.VMEM((rows, channels), jnp.float32)

    sems = pltpu.SemaphoreType.DMA((2 * len(sizes),))
    out = pl.pallas_call(
        functools.partial(kernel, n, sizes),
        out_shape=buffer(steps),
        in_specs=[pl.BlockSpec(memory_space=pl.ANY)] * 2,
        out_specs=pl.BlockSpec(memory_space=pltpu.VMEM),
        scratch_shapes=[buffer(steps)] * 3
        + [buffer(steps // 2), buffer(tap_gain.shape[0]), pltpu.SemaphoreType.DMA]
        + [sems] * 5
        + [buffer(sizes[DETOUR]), pltpu.SemaphoreType.DMA, pltpu.SemaphoreType.DMA],
        compiler_params=pltpu.CompilerParams(
            collective_id=0, has_side_effects=True, vmem_limit_bytes=52 * 2**20
        ),
        name="echo",
    )(signal, tap_gain)
    return out.reshape(signal.shape)


def solution(mesh):
    in_specs = (P("track", "lane", None, None), P())
    out_specs = P("track", "lane", None, None)
    body = functools.partial(local, mesh.shape["track"])
    return jax.shard_map(body, mesh=mesh, in_specs=in_specs, out_specs=out_specs, check_vma=False)
```

```python
import functools

import jax
import jax.numpy as jnp
from jax import lax
from jax.experimental import pallas as pl
from jax.experimental.pallas import tpu as pltpu
from jax.sharding import PartitionSpec as P

SHARES = (16, 24, 32, 32, 8, 2, 2, 6, 4, 2)
LAG = 1
DETOURS = (5, 6)


def kernel(n, sizes, signal, gain, out, own, near, far, part, gains, gain_sem, load_sem, near_send, near_recv, far_send, far_recv, aside, aside_send, aside_recv, over, over_send, over_recv, via, via_send, via_recv):
    half = own.shape[0] // 2
    count = len(sizes)
    starts = [sum(sizes[:i]) for i in range(count)]
    t = lax.axis_index("track")
    odd = t % 2
    raw_half = odd
    sum_half = 1 - odd
    far_to = 3 - 4 * odd
    far_from = 1 - 4 * odd

    cross = t % 4 // 2
    up = t // 4 % 2
    ending = t // (n - 2)
    helper = (t // (n - 6)) * (1 - t // (n - 4))
    second = (t // (n - 8)) * (1 - t // (n - 6))

    def device(offset):
        return {"track": (t + offset + n) % n}

    barrier = pltpu.get_barrier_semaphore()

    def greet(source):
        pl.semaphore_signal(barrier, inc=1, device_id=device(source), device_id_type=pl.DeviceIdType.MESH)

    greet(-1)
    greet(far_from)

    @pl.when(cross == 1)
    def _():
        greet(-4)

        @pl.when(up == 0)
        def _():
            greet(4)

    @pl.when(cross == 0)
    def _():
        greet(3 - 2 * odd)

    @pl.when(second == 1)
    def _():
        greet(3 - 2 * odd)

    def rows(side, i):
        return pl.ds(pl.multiple_of(side * half + starts[i], 8), sizes[i])

    def near_copy(src, src_rows, side, i):
        return pltpu.make_async_remote_copy(
            src_ref=src.at[src_rows],
            dst_ref=near.at[rows(side, i)],
            send_sem=near_send.at[side * count + i],
            recv_sem=near_recv.at[side * count + i],
            device_id=device(1),
            device_id_type=pl.DeviceIdType.MESH,
        )

    def near_raw(i):
        return near_copy(own, rows(raw_half, i), raw_half, i)

    def near_sum(i):
        return near_copy(part, pl.ds(starts[i], sizes[i]), sum_half, i)

    def far_copy(src, side, i):
        return pltpu.make_async_remote_copy(
            src_ref=src.at[rows(side, i)],
            dst_ref=far.at[rows(side, i)],
            send_sem=far_send.at[side * count + i],
            recv_sem=far_recv.at[side * count + i],
            device_id=device(far_to),
            device_id_type=pl.DeviceIdType.MESH,
        )

    def inner(i):
        return pl.ds(starts[i], sizes[i])

    def over_copy(src, src_rows, send_sem, i, offset):
        return pltpu.make_async_remote_copy(
            src_ref=src.at[src_rows],
            dst_ref=over.at[inner(i)],
            send_sem=send_sem.at[i],
            recv_sem=over_recv.at[i],
            device_id=device(offset),
            device_id_type=pl.DeviceIdType.MESH,
        )

    def via_copy(src, src_rows, send_sem, i):
        return pltpu.make_async_remote_copy(
            src_ref=src.at[src_rows],
            dst_ref=via.at[inner(i)],
            send_sem=send_sem.at[i],
            recv_sem=via_recv.at[i],
            device_id=device(-4),
            device_id_type=pl.DeviceIdType.MESH,
        )

    def leave_row(src, src_rows, send_sem, i):
        @pl.when(up == 0)
        def _():
            over_copy(src, src_rows, send_sem, i, 4).start()

        @pl.when(up == 1)
        def _():
            via_copy(src, src_rows, send_sem, i).start()

    def change_plane(i):
        @pl.when(cross * (1 - up) == 1)
        def _():
            via_copy(via, inner(i), via_send, i).wait_recv()
            over_copy(via, inner(i), via_send, i, 8).start()

    def landing_copy(dst, recv_sem, i):
        return pltpu.make_async_remote_copy(
            src_ref=over.at[inner(i)],
            dst_ref=dst.at[rows(0, i)],
            send_sem=over_send.at[i],
            recv_sem=recv_sem.at[i],
            device_id=device(-1 - 2 * odd),
            device_id_type=pl.DeviceIdType.MESH,
        )

    def land(i):
        @pl.when(cross == 1)
        def _():
            over_copy(over, inner(i), over_send, i, 4).wait_recv()

        @pl.when(cross * odd == 1)
        def _():
            landing_copy(near, near_recv, i).start()

        @pl.when(cross * (1 - odd) == 1)
        def _():
            landing_copy(far, far_recv, i).start()

    def parked(j):
        return pl.ds(j * sizes[DETOURS[0]], sizes[DETOURS[j]])

    def aside_copy(src, j, send_sem, offset):
        return pltpu.make_async_remote_copy(
            src_ref=src,
            dst_ref=aside.at[parked(j)],
            send_sem=send_sem,
            recv_sem=aside_recv.at[j],
            device_id=device(offset),
            device_id_type=pl.DeviceIdType.MESH,
        )

    def back_copy(dst, recv_sem, j, offset):
        return pltpu.make_async_remote_copy(
            src_ref=aside.at[parked(j)],
            dst_ref=dst.at[rows(1, DETOURS[j])],
            send_sem=aside_send.at[j],
            recv_sem=recv_sem.at[count + DETOURS[j]],
            device_id=device(offset),
            device_id_type=pl.DeviceIdType.MESH,
        )

    def onward_copy():
        return aside_copy(aside.at[parked(1)], 1, aside_send.at[1], -1 - 2 * odd)

    def leave_aside(send_sem):
        for j, i in enumerate(DETOURS):
            aside_copy(signal.at[0, 0, rows(1, i)], j, send_sem.at[count + i], -4).start()

    def start(copy, i, way):
        if i not in DETOURS:
            copy.start()
            return

        @pl.when(way == 0)
        def _():
            copy.start()

    def load(side, i):
        at = rows(side, i)
        return pltpu.make_async_copy(signal.at[0, 0, at], own.at[at], load_sem.at[side * count + i])

    for i in range(count):
        load(raw_half, i).start()
        load(sum_half, i).start()
    gain_load = pltpu.make_async_copy(gain, gains, gain_sem)
    gain_load.start()
    pl.semaphore_wait(barrier, 2 + cross * (2 + up) + helper)

    near_copy(signal.at[0, 0], rows(raw_half, 0), raw_half, 0).start()
    far_copy(signal.at[0, 0], sum_half, 0).start()

    @pl.when(ending * odd == 1)
    def _():
        leave_aside(near_send)

    @pl.when(ending * (1 - odd) == 1)
    def _():
        leave_aside(far_send)

    @pl.when(helper == 1)
    def _():
        for j in range(2):
            aside_copy(aside.at[parked(j)], j, aside_send.at[j], -4).wait_recv()
        onward_copy().start()

    @pl.when(helper * odd == 1)
    def _():
        back_copy(near, near_recv, 0, 5).start()

    @pl.when(helper * (1 - odd) == 1)
    def _():
        back_copy(far, far_recv, 0, 7).start()

    for i in range(1, count):
        load(raw_half, i).wait()
        start(near_raw(i), i, ending * odd)
        load(sum_half, i).wait()
        start(far_copy(own, sum_half, i), i, ending * (1 - odd))

    gain_load.wait()
    load(raw_half, 0).wait()
    load(sum_half, 0).wait()
    g0, g1, g2 = gains[0:1], gains[1:2], gains[2:3]

    def blocks(side, i, body):
        block = 64 if sizes[i] % 64 == 0 else 16

        def step(j, _):
            offset = starts[i] + j * block
            body(pl.ds(pl.multiple_of(side * half + offset, 8), block), pl.ds(pl.multiple_of(offset, 8), block))
            return 0

        lax.fori_loop(0, sizes[i] // block, step, 0)

    def add_up(at, inner):
        mine, before = own[at], near[at]
        part[inner] = g1 * mine + g2 * before
        out[at] = g0 * mine + g1 * before

    def finish_raw(at, _):
        out[at] = jnp.tanh(g0 * own[at] + near[at])

    def finish_sum(at, _):
        out[at] = jnp.tanh(out[at] + g2 * far[at])

    for i in range(count):
        near_sum(i).wait_recv()
        blocks(sum_half, i, add_up)
        far_copy(far, raw_half, i).wait_recv()

        @pl.when(cross * (1 - odd) == 0)
        def _():
            far_copy(far, raw_half, i).start()

        @pl.when(cross * (1 - odd) == 1)
        def _():
            leave_row(far, rows(0, i), far_send, i)

        @pl.when(cross * odd == 0)
        def _():
            near_sum(i).start()

        @pl.when(cross * odd == 1)
        def _():
            leave_row(part, inner(i), near_send, i)

        if i >= LAG:
            change_plane(i - LAG)
        if i >= 2 * LAG:
            land(i - 2 * LAG)
        if i == 1:

            @pl.when(second == 1)
            def _():
                onward_copy().wait_recv()

            @pl.when(second * (1 - odd) == 1)
            def _():
                back_copy(near, near_recv, 1, 8).start()

            @pl.when(second * odd == 1)
            def _():
                back_copy(far, far_recv, 1, 8).start()

    for i in range(count - LAG, count):
        change_plane(i)
    for i in range(count - 2 * LAG, count):
        land(i)

    for i in range(count):
        near_raw(i).wait_recv()
        blocks(raw_half, i, finish_raw)
        far_copy(far, sum_half, i).wait_recv()
        blocks(sum_half, i, finish_sum)

    for i in range(count):
        near_raw(i).wait_send()
        near_sum(i).wait_send()
        far_copy(own, sum_half, i).wait_send()
        far_copy(far, raw_half, i).wait_send()

        @pl.when(cross == 1)
        def _():
            landing_copy(far, far_recv, i).wait_send()

        @pl.when(cross * (1 - up) == 1)
        def _():
            over_copy(via, inner(i), via_send, i, 8).wait_send()

    @pl.when(helper == 1)
    def _():
        back_copy(far, far_recv, 0, 7).wait_send()

    @pl.when(helper + second == 1)
    def _():
        back_copy(far, far_recv, 1, 8).wait_send()


def local(n, signal, tap_gain):
    steps, channels = signal.shape[2:]
    sizes = [steps // 2 * share // sum(SHARES) for share in SHARES]

    def buffer(rows):
        return pltpu.VMEM((rows, channels), jnp.float32)

    few = pltpu.SemaphoreType.DMA((len(sizes),))
    sems = pltpu.SemaphoreType.DMA((2 * len(sizes),))
    out = pl.pallas_call(
        functools.partial(kernel, n, sizes),
        out_shape=buffer(steps),
        in_specs=[pl.BlockSpec(memory_space=pl.ANY)] * 2,
        out_specs=pl.BlockSpec(memory_space=pltpu.VMEM),
        scratch_shapes=[buffer(steps)] * 3
        + [buffer(steps // 2), buffer(tap_gain.shape[0]), pltpu.SemaphoreType.DMA]
        + [sems] * 5
        + [buffer(2 * sizes[DETOURS[0]]), pltpu.SemaphoreType.DMA((2,)), pltpu.SemaphoreType.DMA((2,))]
        + [buffer(steps // 2), few, few] * 2,
        compiler_params=pltpu.CompilerParams(
            collective_id=0, has_side_effects=True, vmem_limit_bytes=52 * 2**20
        ),
        name="echo",
    )(signal, tap_gain)
    return out.reshape(signal.shape)


def solution(mesh):
    in_specs = (P("track", "lane", None, None), P())
    out_specs = P("track", "lane", None, None)
    body = functools.partial(local, mesh.shape["track"])
    return jax.shard_map(body, mesh=mesh, in_specs=in_specs, out_specs=out_specs, check_vma=False)
```

```python
import functools

import jax
import jax.numpy as jnp
from jax import lax
from jax.experimental import pallas as pl
from jax.experimental.pallas import tpu as pltpu
from jax.sharding import PartitionSpec as P

SHARES = (8, 16, 28, 34, 22, 2, 1, 9, 5, 3)
LAG = 1
DETOURS = (5, 6)


def kernel(n, sizes, signal, gain, out, own, near, far, part, gains, gain_sem, load_sem, near_send, near_recv, far_send, far_recv, aside, aside_send, aside_recv, over, over_send, over_recv, via, via_send, via_recv):
    half = own.shape[0] // 2
    count = len(sizes)
    starts = [sum(sizes[:i]) for i in range(count)]
    t = lax.axis_index("track")
    odd = t % 2
    raw_half = odd
    sum_half = 1 - odd
    far_to = 3 - 4 * odd
    far_from = 1 - 4 * odd

    cross = t % 4 // 2
    up = t // 4 % 2
    ending = t // (n - 2)
    helper = (t // (n - 6)) * (1 - t // (n - 4))
    second = (t // (n - 8)) * (1 - t // (n - 6))

    def device(offset):
        return {"track": (t + offset + n) % n}

    barrier = pltpu.get_barrier_semaphore()

    def greet(source):
        pl.semaphore_signal(barrier, inc=1, device_id=device(source), device_id_type=pl.DeviceIdType.MESH)

    greet(-1)
    greet(far_from)

    @pl.when(cross == 1)
    def _():
        greet(-4)

        @pl.when(up == 0)
        def _():
            greet(4)

    @pl.when(cross == 0)
    def _():
        greet(3 - 2 * odd)

    @pl.when(second == 1)
    def _():
        greet(3 - 2 * odd)

    def rows(side, i):
        return pl.ds(pl.multiple_of(side * half + starts[i], 8), sizes[i])

    def near_copy(src, src_rows, side, i):
        return pltpu.make_async_remote_copy(
            src_ref=src.at[src_rows],
            dst_ref=near.at[rows(side, i)],
            send_sem=near_send,
            recv_sem=near_recv.at[side * count + i],
            device_id=device(1),
            device_id_type=pl.DeviceIdType.MESH,
        )

    def near_raw(i):
        return near_copy(own, rows(raw_half, i), raw_half, i)

    def near_sum(i):
        return near_copy(part, pl.ds(starts[i], sizes[i]), sum_half, i)

    def far_copy(src, side, i):
        return pltpu.make_async_remote_copy(
            src_ref=src.at[rows(side, i)],
            dst_ref=far.at[rows(side, i)],
            send_sem=far_send,
            recv_sem=far_recv.at[side * count + i],
            device_id=device(far_to),
            device_id_type=pl.DeviceIdType.MESH,
        )

    def inner(i):
        return pl.ds(starts[i], sizes[i])

    def over_copy(src, src_rows, send_sem, i, offset):
        return pltpu.make_async_remote_copy(
            src_ref=src.at[src_rows],
            dst_ref=over.at[inner(i)],
            send_sem=send_sem,
            recv_sem=over_recv.at[i],
            device_id=device(offset),
            device_id_type=pl.DeviceIdType.MESH,
        )

    def via_copy(src, src_rows, send_sem, i):
        return pltpu.make_async_remote_copy(
            src_ref=src.at[src_rows],
            dst_ref=via.at[inner(i)],
            send_sem=send_sem,
            recv_sem=via_recv.at[i],
            device_id=device(-4),
            device_id_type=pl.DeviceIdType.MESH,
        )

    def leave_row(src, src_rows, send_sem, i):
        @pl.when(up == 0)
        def _():
            over_copy(src, src_rows, send_sem, i, 4).start()

        @pl.when(up == 1)
        def _():
            via_copy(src, src_rows, send_sem, i).start()

    def change_plane(i):
        @pl.when(cross * (1 - up) == 1)
        def _():
            via_copy(via, inner(i), via_send, i).wait_recv()
            over_copy(via, inner(i), via_send, i, 8).start()

    def landing_copy(dst, recv_sem, i):
        return pltpu.make_async_remote_copy(
            src_ref=over.at[inner(i)],
            dst_ref=dst.at[rows(0, i)],
            send_sem=over_send,
            recv_sem=recv_sem.at[i],
            device_id=device(-1 - 2 * odd),
            device_id_type=pl.DeviceIdType.MESH,
        )

    def land(i):
        @pl.when(cross == 1)
        def _():
            over_copy(over, inner(i), over_send, i, 4).wait_recv()

        @pl.when(cross * odd == 1)
        def _():
            landing_copy(near, near_recv, i).start()

        @pl.when(cross * (1 - odd) == 1)
        def _():
            landing_copy(far, far_recv, i).start()

    def parked(j):
        return pl.ds(j * sizes[DETOURS[0]], sizes[DETOURS[j]])

    def aside_copy(src, j, send_sem, offset):
        return pltpu.make_async_remote_copy(
            src_ref=src,
            dst_ref=aside.at[parked(j)],
            send_sem=send_sem,
            recv_sem=aside_recv.at[j],
            device_id=device(offset),
            device_id_type=pl.DeviceIdType.MESH,
        )

    def back_copy(dst, recv_sem, j, offset):
        return pltpu.make_async_remote_copy(
            src_ref=aside.at[parked(j)],
            dst_ref=dst.at[rows(1, DETOURS[j])],
            send_sem=aside_send.at[j],
            recv_sem=recv_sem.at[count + DETOURS[j]],
            device_id=device(offset),
            device_id_type=pl.DeviceIdType.MESH,
        )

    def onward_copy():
        return aside_copy(aside.at[parked(1)], 1, aside_send.at[1], -1 - 2 * odd)

    def leave_aside(send_sem):
        for j, i in enumerate(DETOURS):
            aside_copy(signal.at[0, 0, rows(1, i)], j, send_sem, -4).start()

    def start(copy, i, way):
        if i not in DETOURS:
            copy.start()
            return

        @pl.when(way == 0)
        def _():
            copy.start()

    def load(side, i):
        at = rows(side, i)
        return pltpu.make_async_copy(signal.at[0, 0, at], own.at[at], load_sem.at[side * count + i])

    for i in range(count):
        load(raw_half, i).start()
        load(sum_half, i).start()
    gain_load = pltpu.make_async_copy(gain, gains, gain_sem)
    gain_load.start()
    pl.semaphore_wait(barrier, 2 + cross * (2 + up) + helper)

    near_copy(signal.at[0, 0], rows(raw_half, 0), raw_half, 0).start()
    far_copy(signal.at[0, 0], sum_half, 0).start()

    @pl.when(ending * odd == 1)
    def _():
        leave_aside(near_send)

    @pl.when(ending * (1 - odd) == 1)
    def _():
        leave_aside(far_send)

    @pl.when(helper == 1)
    def _():
        for j in range(2):
            aside_copy(aside.at[parked(j)], j, aside_send.at[j], -4).wait_recv()
        onward_copy().start()

    @pl.when(helper * odd == 1)
    def _():
        back_copy(near, near_recv, 0, 5).start()

    @pl.when(helper * (1 - odd) == 1)
    def _():
        back_copy(far, far_recv, 0, 7).start()

    for i in range(1, count):
        load(raw_half, i).wait()
        start(near_raw(i), i, ending * odd)
        load(sum_half, i).wait()
        start(far_copy(own, sum_half, i), i, ending * (1 - odd))

    gain_load.wait()
    load(raw_half, 0).wait()
    load(sum_half, 0).wait()
    g0, g1, g2 = gains[0:1], gains[1:2], gains[2:3]

    def blocks(side, i, body):
        block = 64 if sizes[i] % 64 == 0 else 16

        def step(j, _):
            offset = starts[i] + j * block
            body(pl.ds(pl.multiple_of(side * half + offset, 8), block), pl.ds(pl.multiple_of(offset, 8), block))
            return 0

        lax.fori_loop(0, sizes[i] // block, step, 0)

    def add_up(at, inner):
        mine, before = own[at], near[at]
        part[inner] = g1 * mine + g2 * before
        out[at] = g0 * mine + g1 * before

    def finish_raw(at, _):
        out[at] = jnp.tanh(g0 * own[at] + near[at])

    def finish_sum(at, _):
        out[at] = jnp.tanh(out[at] + g2 * far[at])

    for i in range(count):
        near_sum(i).wait_recv()
        blocks(sum_half, i, add_up)
        far_copy(far, raw_half, i).wait_recv()

        @pl.when(cross * (1 - odd) == 0)
        def _():
            far_copy(far, raw_half, i).start()

        @pl.when(cross * (1 - odd) == 1)
        def _():
            leave_row(far, rows(0, i), far_send, i)

        @pl.when(cross * odd == 0)
        def _():
            near_sum(i).start()

        @pl.when(cross * odd == 1)
        def _():
            leave_row(part, inner(i), near_send, i)

        if i >= LAG:
            change_plane(i - LAG)
        if i >= 2 * LAG:
            land(i - 2 * LAG)
        if i == 1:

            @pl.when(second == 1)
            def _():
                onward_copy().wait_recv()

            @pl.when(second * (1 - odd) == 1)
            def _():
                back_copy(near, near_recv, 1, 8).start()

            @pl.when(second * odd == 1)
            def _():
                back_copy(far, far_recv, 1, 8).start()

    for i in range(count - LAG, count):
        change_plane(i)
    for i in range(count - 2 * LAG, count):
        land(i)

    for i in range(count):
        near_raw(i).wait_recv()
        blocks(raw_half, i, finish_raw)
        far_copy(far, sum_half, i).wait_recv()
        blocks(sum_half, i, finish_sum)

    def sent(buffer, send_sem, recv_sem):
        pltpu.make_async_remote_copy(
            src_ref=buffer,
            dst_ref=buffer,
            send_sem=send_sem,
            recv_sem=recv_sem.at[0],
            device_id=device(1),
            device_id_type=pl.DeviceIdType.MESH,
        ).wait_send()

    sent(near, near_send, near_recv)
    sent(far, far_send, far_recv)

    @pl.when(cross == 1)
    def _():
        sent(over, over_send, over_recv)

    @pl.when(cross * (1 - up) == 1)
    def _():
        sent(via, via_send, via_recv)

    @pl.when(helper == 1)
    def _():
        back_copy(far, far_recv, 0, 7).wait_send()

    @pl.when(helper + second == 1)
    def _():
        back_copy(far, far_recv, 1, 8).wait_send()


def local(n, signal, tap_gain):
    steps, channels = signal.shape[2:]
    sizes = [steps // 2 * share // sum(SHARES) for share in SHARES]

    def buffer(rows):
        return pltpu.VMEM((rows, channels), jnp.float32)

    one = pltpu.SemaphoreType.DMA
    few = pltpu.SemaphoreType.DMA((len(sizes),))
    sems = pltpu.SemaphoreType.DMA((2 * len(sizes),))
    out = pl.pallas_call(
        functools.partial(kernel, n, sizes),
        out_shape=buffer(steps),
        in_specs=[pl.BlockSpec(memory_space=pl.ANY)] * 2,
        out_specs=pl.BlockSpec(memory_space=pltpu.VMEM),
        scratch_shapes=[buffer(steps)] * 3
        + [buffer(steps // 2), buffer(tap_gain.shape[0]), one]
        + [sems, one, sems, one, sems]
        + [buffer(2 * sizes[DETOURS[0]]), pltpu.SemaphoreType.DMA((2,)), pltpu.SemaphoreType.DMA((2,))]
        + [buffer(steps // 2), one, few] * 2,
        compiler_params=pltpu.CompilerParams(
            collective_id=0, has_side_effects=True, vmem_limit_bytes=52 * 2**20
        ),
        name="echo",
    )(signal, tap_gain)
    return out.reshape(signal.shape)


def solution(mesh):
    in_specs = (P("track", "lane", None, None), P())
    out_specs = P("track", "lane", None, None)
    body = functools.partial(local, mesh.shape["track"])
    return jax.shard_map(body, mesh=mesh, in_specs=in_specs, out_specs=out_specs, check_vma=False)
```

```python
import functools

import jax
import jax.numpy as jnp
from jax import lax
from jax.experimental import pallas as pl
from jax.experimental.pallas import tpu as pltpu
from jax.sharding import PartitionSpec as P

SHARES = (8, 16, 28, 34, 22, 2, 1, 9, 5, 3)
LAG = 1
DETOURS = (5, 6)


def kernel(n, sizes, signal, gain, out, own, near, far, part, gains, gain_sem, load_sem, near_send, near_recv, far_send, far_recv, aside, aside_send, aside_recv, over, over_send, over_recv, via, via_send, via_recv):
    half = own.shape[0] // 2
    count = len(sizes)
    starts = [sum(sizes[:i]) for i in range(count)]
    t = lax.axis_index("track")
    odd = t % 2
    raw_half = odd
    sum_half = 1 - odd
    far_to = 3 - 4 * odd
    far_from = 1 - 4 * odd

    cross = t % 4 // 2
    up = t // 4 % 2
    ending = t // (n - 2)
    helper = (t // (n - 6)) * (1 - t // (n - 4))
    second = (t // (n - 8)) * (1 - t // (n - 6))

    def device(offset):
        return {"track": (t + offset + n) % n}

    barrier = pltpu.get_barrier_semaphore()

    def greet(source):
        pl.semaphore_signal(barrier, inc=1, device_id=device(source), device_id_type=pl.DeviceIdType.MESH)

    greet(-1)
    greet(far_from)

    @pl.when(cross == 1)
    def _():
        greet(-4)

        @pl.when(up == 0)
        def _():
            greet(4)

    @pl.when(cross == 0)
    def _():
        greet(3 - 2 * odd)

    @pl.when(second == 1)
    def _():
        greet(3 - 2 * odd)

    def rows(side, i):
        return pl.ds(pl.multiple_of(side * half + starts[i], 8), sizes[i])

    def near_copy(src, src_rows, side, i):
        return pltpu.make_async_remote_copy(
            src_ref=src.at[src_rows],
            dst_ref=near.at[rows(side, i)],
            send_sem=near_send,
            recv_sem=near_recv.at[side * count + i],
            device_id=device(1),
            device_id_type=pl.DeviceIdType.MESH,
        )

    def near_raw(i):
        return near_copy(own, rows(raw_half, i), raw_half, i)

    def near_sum(i):
        return near_copy(part, pl.ds(starts[i], sizes[i]), sum_half, i)

    def far_copy(src, side, i):
        return pltpu.make_async_remote_copy(
            src_ref=src.at[rows(side, i)],
            dst_ref=far.at[rows(side, i)],
            send_sem=far_send,
            recv_sem=far_recv.at[side * count + i],
            device_id=device(far_to),
            device_id_type=pl.DeviceIdType.MESH,
        )

    def inner(i):
        return pl.ds(starts[i], sizes[i])

    def over_copy(src, src_rows, send_sem, i, offset):
        return pltpu.make_async_remote_copy(
            src_ref=src.at[src_rows],
            dst_ref=over.at[inner(i)],
            send_sem=send_sem,
            recv_sem=over_recv.at[i],
            device_id=device(offset),
            device_id_type=pl.DeviceIdType.MESH,
        )

    def via_copy(src, src_rows, send_sem, i):
        return pltpu.make_async_remote_copy(
            src_ref=src.at[src_rows],
            dst_ref=via.at[inner(i)],
            send_sem=send_sem,
            recv_sem=via_recv.at[i],
            device_id=device(-4),
            device_id_type=pl.DeviceIdType.MESH,
        )

    def leave_row(src, src_rows, send_sem, i):
        @pl.when(up == 0)
        def _():
            over_copy(src, src_rows, send_sem, i, 4).start()

        @pl.when(up == 1)
        def _():
            via_copy(src, src_rows, send_sem, i).start()

    def change_plane(i):
        @pl.when(cross * (1 - up) == 1)
        def _():
            via_copy(via, inner(i), via_send, i).wait_recv()
            over_copy(via, inner(i), via_send, i, 8).start()

    def landing_copy(dst, recv_sem, i):
        return pltpu.make_async_remote_copy(
            src_ref=over.at[inner(i)],
            dst_ref=dst.at[rows(0, i)],
            send_sem=over_send,
            recv_sem=recv_sem.at[i],
            device_id=device(-1 - 2 * odd),
            device_id_type=pl.DeviceIdType.MESH,
        )

    def land(i):
        @pl.when(cross == 1)
        def _():
            over_copy(over, inner(i), over_send, i, 4).wait_recv()

        @pl.when(cross * odd == 1)
        def _():
            landing_copy(near, near_recv, i).start()

        @pl.when(cross * (1 - odd) == 1)
        def _():
            landing_copy(far, far_recv, i).start()

    def parked(j):
        return pl.ds(j * sizes[DETOURS[0]], sizes[DETOURS[j]])

    def aside_copy(src, j, send_sem, offset):
        return pltpu.make_async_remote_copy(
            src_ref=src,
            dst_ref=aside.at[parked(j)],
            send_sem=send_sem,
            recv_sem=aside_recv.at[j],
            device_id=device(offset),
            device_id_type=pl.DeviceIdType.MESH,
        )

    def back_copy(dst, recv_sem, j, offset):
        return pltpu.make_async_remote_copy(
            src_ref=aside.at[parked(j)],
            dst_ref=dst.at[rows(1, DETOURS[j])],
            send_sem=aside_send.at[j],
            recv_sem=recv_sem.at[count + DETOURS[j]],
            device_id=device(offset),
            device_id_type=pl.DeviceIdType.MESH,
        )

    def onward_copy():
        return aside_copy(aside.at[parked(1)], 1, aside_send.at[1], -1 - 2 * odd)

    def leave_aside(send_sem):
        for j, i in enumerate(DETOURS):
            aside_copy(signal.at[0, 0, rows(1, i)], j, send_sem, -4).start()

    def start(copy, i, way):
        if i not in DETOURS:
            copy.start()
            return

        @pl.when(way == 0)
        def _():
            copy.start()

    def load(side, i):
        at = rows(side, i)
        return pltpu.make_async_copy(signal.at[0, 0, at], own.at[at], load_sem.at[side * count + i])

    for i in range(count):
        load(raw_half, i).start()
        load(sum_half, i).start()
    gain_load = pltpu.make_async_copy(gain, gains, gain_sem)
    gain_load.start()
    pl.semaphore_wait(barrier, 2 + cross * (2 + up) + helper)

    near_copy(signal.at[0, 0], rows(raw_half, 0), raw_half, 0).start()
    far_copy(signal.at[0, 0], sum_half, 0).start()

    @pl.when(ending * odd == 1)
    def _():
        leave_aside(near_send)

    @pl.when(ending * (1 - odd) == 1)
    def _():
        leave_aside(far_send)

    @pl.when(helper == 1)
    def _():
        for j in range(2):
            aside_copy(aside.at[parked(j)], j, aside_send.at[j], -4).wait_recv()
        onward_copy().start()

    @pl.when(helper * odd == 1)
    def _():
        back_copy(near, near_recv, 0, 5).start()

    @pl.when(helper * (1 - odd) == 1)
    def _():
        back_copy(far, far_recv, 0, 7).start()

    for i in range(1, count):
        load(raw_half, i).wait()
        start(near_raw(i), i, ending * odd)
        load(sum_half, i).wait()
        start(far_copy(own, sum_half, i), i, ending * (1 - odd))

    gain_load.wait()
    load(raw_half, 0).wait()
    load(sum_half, 0).wait()
    g0, g1, g2 = gains[0:1], gains[1:2], gains[2:3]

    def blocks(side, i, body):
        block = next(b for b in (64, 48, 32, 16) if sizes[i] % b == 0)

        def step(j, _):
            offset = starts[i] + j * block
            body(pl.ds(pl.multiple_of(side * half + offset, 8), block), pl.ds(pl.multiple_of(offset, 8), block))
            return 0

        lax.fori_loop(0, sizes[i] // block, step, 0)

    def add_up(at, inner):
        mine, before = own[at], near[at]
        part[inner] = g1 * mine + g2 * before
        out[at] = g0 * mine + g1 * before

    def finish_raw(at, _):
        out[at] = jnp.tanh(g0 * own[at] + near[at])

    def finish_sum(at, _):
        out[at] = jnp.tanh(out[at] + g2 * far[at])

    for i in range(count):
        near_sum(i).wait_recv()
        blocks(sum_half, i, add_up)
        far_copy(far, raw_half, i).wait_recv()

        @pl.when(cross * (1 - odd) == 0)
        def _():
            far_copy(far, raw_half, i).start()

        @pl.when(cross * (1 - odd) == 1)
        def _():
            leave_row(far, rows(0, i), far_send, i)

        @pl.when(cross * odd == 0)
        def _():
            near_sum(i).start()

        @pl.when(cross * odd == 1)
        def _():
            leave_row(part, inner(i), near_send, i)

        if i >= LAG:
            change_plane(i - LAG)
        if i >= 2 * LAG:
            land(i - 2 * LAG)
        if i == 1:

            @pl.when(second == 1)
            def _():
                onward_copy().wait_recv()

            @pl.when(second * (1 - odd) == 1)
            def _():
                back_copy(near, near_recv, 1, 8).start()

            @pl.when(second * odd == 1)
            def _():
                back_copy(far, far_recv, 1, 8).start()

    for i in range(count - LAG, count):
        change_plane(i)
    for i in range(count - 2 * LAG, count):
        land(i)

    for i in range(count - 1):
        near_raw(i).wait_recv()
        blocks(raw_half, i, finish_raw)
        far_copy(far, sum_half, i).wait_recv()
        blocks(sum_half, i, finish_sum)
    far_copy(far, sum_half, count - 1).wait_recv()
    blocks(sum_half, count - 1, finish_sum)
    near_raw(count - 1).wait_recv()
    blocks(raw_half, count - 1, finish_raw)

    def sent(buffer, send_sem, recv_sem):
        pltpu.make_async_remote_copy(
            src_ref=buffer,
            dst_ref=buffer,
            send_sem=send_sem,
            recv_sem=recv_sem.at[0],
            device_id=device(1),
            device_id_type=pl.DeviceIdType.MESH,
        ).wait_send()

    sent(near, near_send, near_recv)
    sent(far, far_send, far_recv)

    @pl.when(cross == 1)
    def _():
        sent(over, over_send, over_recv)

    @pl.when(cross * (1 - up) == 1)
    def _():
        sent(via, via_send, via_recv)

    @pl.when(helper == 1)
    def _():
        back_copy(far, far_recv, 0, 7).wait_send()

    @pl.when(helper + second == 1)
    def _():
        back_copy(far, far_recv, 1, 8).wait_send()


def local(n, signal, tap_gain):
    steps, channels = signal.shape[2:]
    sizes = [steps // 2 * share // sum(SHARES) for share in SHARES]

    def buffer(rows):
        return pltpu.VMEM((rows, channels), jnp.float32)

    one = pltpu.SemaphoreType.DMA
    few = pltpu.SemaphoreType.DMA((len(sizes),))
    sems = pltpu.SemaphoreType.DMA((2 * len(sizes),))
    out = pl.pallas_call(
        functools.partial(kernel, n, sizes),
        out_shape=buffer(steps),
        in_specs=[pl.BlockSpec(memory_space=pl.ANY)] * 2,
        out_specs=pl.BlockSpec(memory_space=pltpu.VMEM),
        scratch_shapes=[buffer(steps)] * 3
        + [buffer(steps // 2), buffer(tap_gain.shape[0]), one]
        + [sems, one, sems, one, sems]
        + [buffer(2 * sizes[DETOURS[0]]), pltpu.SemaphoreType.DMA((2,)), pltpu.SemaphoreType.DMA((2,))]
        + [buffer(steps // 2), one, few] * 2,
        compiler_params=pltpu.CompilerParams(
            collective_id=0, has_side_effects=True, vmem_limit_bytes=52 * 2**20
        ),
        name="echo",
    )(signal, tap_gain)
    return out.reshape(signal.shape)


def solution(mesh):
    in_specs = (P("track", "lane", None, None), P())
    out_specs = P("track", "lane", None, None)
    body = functools.partial(local, mesh.shape["track"])
    return jax.shard_map(body, mesh=mesh, in_specs=in_specs, out_specs=out_specs, check_vma=False)
```

```python
import functools

import jax
import jax.numpy as jnp
from jax import lax
from jax.experimental import pallas as pl
from jax.experimental.pallas import tpu as pltpu
from jax.sharding import PartitionSpec as P

SHARES = (8, 16, 28, 34, 28, 2, 1, 8, 3)
LAG = 1
DETOURS = (5, 6)


def kernel(n, sizes, signal, gain, out, own, near, far, part, gains, gain_sem, load_sem, near_send, near_recv, far_send, far_recv, aside, aside_send, aside_recv, over, over_send, over_recv, via, via_send, via_recv):
    half = own.shape[0] // 2
    count = len(sizes)
    starts = [sum(sizes[:i]) for i in range(count)]
    t = lax.axis_index("track")
    odd = t % 2
    raw_half = odd
    sum_half = 1 - odd
    far_to = 3 - 4 * odd
    far_from = 1 - 4 * odd

    cross = t % 4 // 2
    up = t // 4 % 2
    ending = t // (n - 2)
    helper = (t // (n - 6)) * (1 - t // (n - 4))
    second = (t // (n - 8)) * (1 - t // (n - 6))

    def device(offset):
        return {"track": (t + offset + n) % n}

    barrier = pltpu.get_barrier_semaphore()

    def greet(source):
        pl.semaphore_signal(barrier, inc=1, device_id=device(source), device_id_type=pl.DeviceIdType.MESH)

    greet(-1)
    greet(far_from)

    @pl.when(cross == 1)
    def _():
        greet(-4)

        @pl.when(up == 0)
        def _():
            greet(4)

    @pl.when(cross == 0)
    def _():
        greet(3 - 2 * odd)

    @pl.when(second == 1)
    def _():
        greet(3 - 2 * odd)

    def rows(side, i):
        return pl.ds(pl.multiple_of(side * half + starts[i], 8), sizes[i])

    def near_copy(src, src_rows, side, i):
        return pltpu.make_async_remote_copy(
            src_ref=src.at[src_rows],
            dst_ref=near.at[rows(side, i)],
            send_sem=near_send,
            recv_sem=near_recv.at[side * count + i],
            device_id=device(1),
            device_id_type=pl.DeviceIdType.MESH,
        )

    def near_raw(i):
        return near_copy(own, rows(raw_half, i), raw_half, i)

    def near_sum(i):
        return near_copy(part, pl.ds(starts[i], sizes[i]), sum_half, i)

    def far_copy(src, side, i):
        return pltpu.make_async_remote_copy(
            src_ref=src.at[rows(side, i)],
            dst_ref=far.at[rows(side, i)],
            send_sem=far_send,
            recv_sem=far_recv.at[side * count + i],
            device_id=device(far_to),
            device_id_type=pl.DeviceIdType.MESH,
        )

    def inner(i):
        return pl.ds(starts[i], sizes[i])

    def over_copy(src, src_rows, send_sem, i, offset):
        return pltpu.make_async_remote_copy(
            src_ref=src.at[src_rows],
            dst_ref=over.at[inner(i)],
            send_sem=send_sem,
            recv_sem=over_recv.at[i],
            device_id=device(offset),
            device_id_type=pl.DeviceIdType.MESH,
        )

    def via_copy(src, src_rows, send_sem, i):
        return pltpu.make_async_remote_copy(
            src_ref=src.at[src_rows],
            dst_ref=via.at[inner(i)],
            send_sem=send_sem,
            recv_sem=via_recv.at[i],
            device_id=device(-4),
            device_id_type=pl.DeviceIdType.MESH,
        )

    def leave_row(src, src_rows, send_sem, i):
        @pl.when(up == 0)
        def _():
            over_copy(src, src_rows, send_sem, i, 4).start()

        @pl.when(up == 1)
        def _():
            via_copy(src, src_rows, send_sem, i).start()

    def change_plane(i):
        @pl.when(cross * (1 - up) == 1)
        def _():
            via_copy(via, inner(i), via_send, i).wait_recv()
            over_copy(via, inner(i), via_send, i, 8).start()

    def landing_copy(dst, recv_sem, i):
        return pltpu.make_async_remote_copy(
            src_ref=over.at[inner(i)],
            dst_ref=dst.at[rows(0, i)],
            send_sem=over_send,
            recv_sem=recv_sem.at[i],
            device_id=device(-1 - 2 * odd),
            device_id_type=pl.DeviceIdType.MESH,
        )

    def land(i):
        @pl.when(cross == 1)
        def _():
            over_copy(over, inner(i), over_send, i, 4).wait_recv()

        @pl.when(cross * odd == 1)
        def _():
            landing_copy(near, near_recv, i).start()

        @pl.when(cross * (1 - odd) == 1)
        def _():
            landing_copy(far, far_recv, i).start()

    def parked(j):
        return pl.ds(j * sizes[DETOURS[0]], sizes[DETOURS[j]])

    def aside_copy(src, j, send_sem, offset):
        return pltpu.make_async_remote_copy(
            src_ref=src,
            dst_ref=aside.at[parked(j)],
            send_sem=send_sem,
            recv_sem=aside_recv.at[j],
            device_id=device(offset),
            device_id_type=pl.DeviceIdType.MESH,
        )

    def back_copy(dst, recv_sem, j, offset):
        return pltpu.make_async_remote_copy(
            src_ref=aside.at[parked(j)],
            dst_ref=dst.at[rows(1, DETOURS[j])],
            send_sem=aside_send.at[j],
            recv_sem=recv_sem.at[count + DETOURS[j]],
            device_id=device(offset),
            device_id_type=pl.DeviceIdType.MESH,
        )

    def onward_copy():
        return aside_copy(aside.at[parked(1)], 1, aside_send.at[1], -1 - 2 * odd)

    def leave_aside(send_sem):
        for j, i in enumerate(DETOURS):
            aside_copy(signal.at[0, 0, rows(1, i)], j, send_sem, -4).start()

    def start(copy, i, way):
        if i not in DETOURS:
            copy.start()
            return

        @pl.when(way == 0)
        def _():
            copy.start()

    def load(side, i):
        at = rows(side, i)
        return pltpu.make_async_copy(signal.at[0, 0, at], own.at[at], load_sem.at[side * count + i])

    for i in range(count):
        load(raw_half, i).start()
        load(sum_half, i).start()
    gain_load = pltpu.make_async_copy(gain, gains, gain_sem)
    gain_load.start()
    pl.semaphore_wait(barrier, 2 + cross * (2 + up) + helper)

    near_copy(signal.at[0, 0], rows(raw_half, 0), raw_half, 0).start()
    far_copy(signal.at[0, 0], sum_half, 0).start()

    @pl.when(ending * odd == 1)
    def _():
        leave_aside(near_send)

    @pl.when(ending * (1 - odd) == 1)
    def _():
        leave_aside(far_send)

    @pl.when(helper == 1)
    def _():
        for j in range(2):
            aside_copy(aside.at[parked(j)], j, aside_send.at[j], -4).wait_recv()
        onward_copy().start()

    @pl.when(helper * odd == 1)
    def _():
        back_copy(near, near_recv, 0, 5).start()

    @pl.when(helper * (1 - odd) == 1)
    def _():
        back_copy(far, far_recv, 0, 7).start()

    for i in range(1, count):
        load(raw_half, i).wait()
        start(near_raw(i), i, ending * odd)
        load(sum_half, i).wait()
        start(far_copy(own, sum_half, i), i, ending * (1 - odd))

    gain_load.wait()
    load(raw_half, 0).wait()
    load(sum_half, 0).wait()
    g0, g1, g2 = gains[0:1], gains[1:2], gains[2:3]

    def blocks(side, i, body):
        block = 64 if sizes[i] % 64 == 0 else 16

        def step(j, _):
            offset = starts[i] + j * block
            body(pl.ds(pl.multiple_of(side * half + offset, 8), block), pl.ds(pl.multiple_of(offset, 8), block))
            return 0

        lax.fori_loop(0, sizes[i] // block, step, 0)

    def add_up(at, inner):
        mine, before = own[at], near[at]
        part[inner] = g1 * mine + g2 * before
        out[at] = g0 * mine + g1 * before

    def finish_raw(at, _):
        out[at] = jnp.tanh(g0 * own[at] + near[at])

    def finish_sum(at, _):
        out[at] = jnp.tanh(out[at] + g2 * far[at])

    for i in range(count):
        near_sum(i).wait_recv()
        blocks(sum_half, i, add_up)
        far_copy(far, raw_half, i).wait_recv()

        @pl.when(cross * (1 - odd) == 0)
        def _():
            far_copy(far, raw_half, i).start()

        @pl.when(cross * (1 - odd) == 1)
        def _():
            leave_row(far, rows(0, i), far_send, i)

        @pl.when(cross * odd == 0)
        def _():
            near_sum(i).start()

        @pl.when(cross * odd == 1)
        def _():
            leave_row(part, inner(i), near_send, i)

        if i >= LAG:
            change_plane(i - LAG)
        if i >= 2 * LAG:
            land(i - 2 * LAG)
        if i == 1:

            @pl.when(second == 1)
            def _():
                onward_copy().wait_recv()

            @pl.when(second * (1 - odd) == 1)
            def _():
                back_copy(near, near_recv, 1, 8).start()

            @pl.when(second * odd == 1)
            def _():
                back_copy(far, far_recv, 1, 8).start()

    for i in range(count - LAG, count):
        change_plane(i)
    for i in range(count - 2 * LAG, count):
        land(i)

    for i in range(count):
        near_raw(i).wait_recv()
        blocks(raw_half, i, finish_raw)
        far_copy(far, sum_half, i).wait_recv()
        blocks(sum_half, i, finish_sum)

    def sent(buffer, send_sem, recv_sem):
        pltpu.make_async_remote_copy(
            src_ref=buffer,
            dst_ref=buffer,
            send_sem=send_sem,
            recv_sem=recv_sem.at[0],
            device_id=device(1),
            device_id_type=pl.DeviceIdType.MESH,
        ).wait_send()

    sent(near, near_send, near_recv)
    sent(far, far_send, far_recv)

    @pl.when(cross == 1)
    def _():
        sent(over, over_send, over_recv)

    @pl.when(cross * (1 - up) == 1)
    def _():
        sent(via, via_send, via_recv)

    @pl.when(helper == 1)
    def _():
        back_copy(far, far_recv, 0, 7).wait_send()

    @pl.when(helper + second == 1)
    def _():
        back_copy(far, far_recv, 1, 8).wait_send()


def local(n, signal, tap_gain):
    steps, channels = signal.shape[2:]
    sizes = [steps // 2 * share // sum(SHARES) for share in SHARES]

    def buffer(rows):
        return pltpu.VMEM((rows, channels), jnp.float32)

    one = pltpu.SemaphoreType.DMA
    few = pltpu.SemaphoreType.DMA((len(sizes),))
    sems = pltpu.SemaphoreType.DMA((2 * len(sizes),))
    out = pl.pallas_call(
        functools.partial(kernel, n, sizes),
        out_shape=buffer(steps),
        in_specs=[pl.BlockSpec(memory_space=pl.ANY)] * 2,
        out_specs=pl.BlockSpec(memory_space=pltpu.VMEM),
        scratch_shapes=[buffer(steps)] * 3
        + [buffer(steps // 2), buffer(tap_gain.shape[0]), one]
        + [sems, one, sems, one, sems]
        + [buffer(2 * sizes[DETOURS[0]]), pltpu.SemaphoreType.DMA((2,)), pltpu.SemaphoreType.DMA((2,))]
        + [buffer(steps // 2), one, few] * 2,
        compiler_params=pltpu.CompilerParams(
            collective_id=0, has_side_effects=True, vmem_limit_bytes=52 * 2**20
        ),
        name="echo",
    )(signal, tap_gain)
    return out.reshape(signal.shape)


def solution(mesh):
    in_specs = (P("track", "lane", None, None), P())
    out_specs = P("track", "lane", None, None)
    body = functools.partial(local, mesh.shape["track"])
    return jax.shard_map(body, mesh=mesh, in_specs=in_specs, out_specs=out_specs, check_vma=False)
```

```python
import functools

import jax
import jax.numpy as jnp
from jax import lax
from jax.experimental import pallas as pl
from jax.experimental.pallas import tpu as pltpu
from jax.sharding import PartitionSpec as P

SHARES = (8, 16, 28, 34, 22, 2, 1, 9, 5, 3)
LAG = 1
DETOURS = (5, 6)


def kernel(n, sizes, signal, gain, out, own, near, far, part, gains, gain_sem, load_sem, near_send, near_recv, far_send, far_recv, aside, aside_send, aside_recv, over, over_send, over_recv, via, via_send, via_recv):
    half = own.shape[0] // 2
    count = len(sizes)
    starts = [sum(sizes[:i]) for i in range(count)]
    t = lax.axis_index("track")
    odd = t % 2
    raw_half = odd
    sum_half = 1 - odd
    far_to = 3 - 4 * odd
    far_from = 1 - 4 * odd

    cross = t % 4 // 2
    up = t // 4 % 2
    ending = t // (n - 2)
    helper = (t // (n - 6)) * (1 - t // (n - 4))
    second = (t // (n - 8)) * (1 - t // (n - 6))

    def device(offset):
        return {"track": (t + offset + n) % n}

    barrier = pltpu.get_barrier_semaphore()

    def greet(source):
        pl.semaphore_signal(barrier, inc=1, device_id=device(source), device_id_type=pl.DeviceIdType.MESH)

    greet(-1)
    greet(far_from)

    @pl.when(cross == 1)
    def _():
        greet(-4)

        @pl.when(up == 0)
        def _():
            greet(4)

    @pl.when(cross == 0)
    def _():
        greet(3 - 2 * odd)

    @pl.when(second == 1)
    def _():
        greet(3 - 2 * odd)

    def rows(side, i):
        return pl.ds(pl.multiple_of(side * half + starts[i], 8), sizes[i])

    def near_copy(src, src_rows, side, i):
        return pltpu.make_async_remote_copy(
            src_ref=src.at[src_rows],
            dst_ref=near.at[rows(side, i)],
            send_sem=near_send,
            recv_sem=near_recv.at[side * count + i],
            device_id=device(1),
            device_id_type=pl.DeviceIdType.MESH,
        )

    def near_raw(i):
        return near_copy(own, rows(raw_half, i), raw_half, i)

    def near_sum(i):
        return near_copy(part, pl.ds(starts[i], sizes[i]), sum_half, i)

    def far_copy(src, side, i):
        return pltpu.make_async_remote_copy(
            src_ref=src.at[rows(side, i)],
            dst_ref=far.at[rows(side, i)],
            send_sem=far_send,
            recv_sem=far_recv.at[side * count + i],
            device_id=device(far_to),
            device_id_type=pl.DeviceIdType.MESH,
        )

    def inner(i):
        return pl.ds(starts[i], sizes[i])

    def over_copy(src, src_rows, send_sem, i, offset):
        return pltpu.make_async_remote_copy(
            src_ref=src.at[src_rows],
            dst_ref=over.at[inner(i)],
            send_sem=send_sem,
            recv_sem=over_recv.at[i],
            device_id=device(offset),
            device_id_type=pl.DeviceIdType.MESH,
        )

    def via_copy(src, src_rows, send_sem, i):
        return pltpu.make_async_remote_copy(
            src_ref=src.at[src_rows],
            dst_ref=via.at[inner(i)],
            send_sem=send_sem,
            recv_sem=via_recv.at[i],
            device_id=device(-4),
            device_id_type=pl.DeviceIdType.MESH,
        )

    def leave_row(src, src_rows, send_sem, i):
        @pl.when(up == 0)
        def _():
            over_copy(src, src_rows, send_sem, i, 4).start()

        @pl.when(up == 1)
        def _():
            via_copy(src, src_rows, send_sem, i).start()

    def change_plane(i):
        @pl.when(cross * (1 - up) == 1)
        def _():
            via_copy(via, inner(i), via_send, i).wait_recv()
            over_copy(via, inner(i), via_send, i, 8).start()

    def landing_copy(dst, recv_sem, i):
        return pltpu.make_async_remote_copy(
            src_ref=over.at[inner(i)],
            dst_ref=dst.at[rows(0, i)],
            send_sem=over_send,
            recv_sem=recv_sem.at[i],
            device_id=device(-1 - 2 * odd),
            device_id_type=pl.DeviceIdType.MESH,
        )

    def land(i):
        @pl.when(cross == 1)
        def _():
            over_copy(over, inner(i), over_send, i, 4).wait_recv()

        @pl.when(cross * odd == 1)
        def _():
            landing_copy(near, near_recv, i).start()

        @pl.when(cross * (1 - odd) == 1)
        def _():
            landing_copy(far, far_recv, i).start()

    def parked(j):
        return pl.ds(j * sizes[DETOURS[0]], sizes[DETOURS[j]])

    def aside_copy(src, j, send_sem, offset):
        return pltpu.make_async_remote_copy(
            src_ref=src,
            dst_ref=aside.at[parked(j)],
            send_sem=send_sem,
            recv_sem=aside_recv.at[j],
            device_id=device(offset),
            device_id_type=pl.DeviceIdType.MESH,
        )

    def back_copy(dst, recv_sem, j, offset):
        return pltpu.make_async_remote_copy(
            src_ref=aside.at[parked(j)],
            dst_ref=dst.at[rows(1, DETOURS[j])],
            send_sem=aside_send.at[j],
            recv_sem=recv_sem.at[count + DETOURS[j]],
            device_id=device(offset),
            device_id_type=pl.DeviceIdType.MESH,
        )

    def onward_copy():
        return aside_copy(aside.at[parked(1)], 1, aside_send.at[1], -1 - 2 * odd)

    def leave_aside(send_sem):
        for j, i in enumerate(DETOURS):
            aside_copy(signal.at[0, 0, rows(1, i)], j, send_sem, -4).start()

    def start(copy, i, way):
        if i not in DETOURS:
            copy.start()
            return

        @pl.when(way == 0)
        def _():
            copy.start()

    def load(side, i):
        at = rows(side, i)
        return pltpu.make_async_copy(signal.at[0, 0, at], own.at[at], load_sem.at[side * count + i])

    for i in range(count):
        load(raw_half, i).start()
        load(sum_half, i).start()
    gain_load = pltpu.make_async_copy(gain, gains, gain_sem)
    gain_load.start()
    pl.semaphore_wait(barrier, 2 + cross * (2 + up) + helper)

    near_copy(signal.at[0, 0], rows(raw_half, 0), raw_half, 0).start()
    far_copy(signal.at[0, 0], sum_half, 0).start()

    @pl.when(ending * odd == 1)
    def _():
        leave_aside(near_send)

    @pl.when(ending * (1 - odd) == 1)
    def _():
        leave_aside(far_send)

    @pl.when(helper == 1)
    def _():
        for j in range(2):
            aside_copy(aside.at[parked(j)], j, aside_send.at[j], -4).wait_recv()
        onward_copy().start()

    @pl.when(helper * odd == 1)
    def _():
        back_copy(near, near_recv, 0, 5).start()

    @pl.when(helper * (1 - odd) == 1)
    def _():
        back_copy(far, far_recv, 0, 7).start()

    for i in range(1, count):
        load(raw_half, i).wait()
        start(near_raw(i), i, ending * odd)
        load(sum_half, i).wait()
        start(far_copy(own, sum_half, i), i, ending * (1 - odd))

    gain_load.wait()
    load(raw_half, 0).wait()
    load(sum_half, 0).wait()
    g0, g1, g2 = gains[0:1], gains[1:2], gains[2:3]

    def blocks(side, i, body):
        block = 64 if sizes[i] % 64 == 0 else 16

        def step(j, _):
            offset = starts[i] + j * block
            body(pl.ds(pl.multiple_of(side * half + offset, 8), block), pl.ds(pl.multiple_of(offset, 8), block))
            return 0

        lax.fori_loop(0, sizes[i] // block, step, 0)

    def add_up(at, inner):
        mine, before = own[at], near[at]
        part[inner] = g1 * mine + g2 * before
        out[at] = g0 * mine + g1 * before

    def finish_raw(at, _):
        out[at] = jnp.tanh(g0 * own[at] + near[at])

    def finish_sum(at, _):
        out[at] = jnp.tanh(out[at] + g2 * far[at])

    for i in range(count):
        near_sum(i).wait_recv()
        blocks(sum_half, i, add_up)
        far_copy(far, raw_half, i).wait_recv()

        @pl.when(cross * (1 - odd) == 0)
        def _():
            far_copy(far, raw_half, i).start()

        @pl.when(cross * (1 - odd) == 1)
        def _():
            leave_row(far, rows(0, i), far_send, i)

        @pl.when(cross * odd == 0)
        def _():
            near_sum(i).start()

        @pl.when(cross * odd == 1)
        def _():
            leave_row(part, inner(i), near_send, i)

        if i >= 2 * LAG:
            land(i - 2 * LAG)
        if i >= LAG:
            change_plane(i - LAG)
        if i == 1:

            @pl.when(second == 1)
            def _():
                onward_copy().wait_recv()

            @pl.when(second * (1 - odd) == 1)
            def _():
                back_copy(near, near_recv, 1, 8).start()

            @pl.when(second * odd == 1)
            def _():
                back_copy(far, far_recv, 1, 8).start()

    for i in range(count - LAG, count):
        change_plane(i)
    for i in range(count - 2 * LAG, count):
        land(i)

    for i in range(count):
        near_raw(i).wait_recv()
        blocks(raw_half, i, finish_raw)
        far_copy(far, sum_half, i).wait_recv()
        blocks(sum_half, i, finish_sum)

    def sent(buffer, send_sem, recv_sem):
        pltpu.make_async_remote_copy(
            src_ref=buffer,
            dst_ref=buffer,
            send_sem=send_sem,
            recv_sem=recv_sem.at[0],
            device_id=device(1),
            device_id_type=pl.DeviceIdType.MESH,
        ).wait_send()

    sent(near, near_send, near_recv)
    sent(far, far_send, far_recv)

    @pl.when(cross == 1)
    def _():
        sent(over, over_send, over_recv)

    @pl.when(cross * (1 - up) == 1)
    def _():
        sent(via, via_send, via_recv)

    @pl.when(helper == 1)
    def _():
        back_copy(far, far_recv, 0, 7).wait_send()

    @pl.when(helper + second == 1)
    def _():
        back_copy(far, far_recv, 1, 8).wait_send()


def local(n, signal, tap_gain):
    steps, channels = signal.shape[2:]
    sizes = [steps // 2 * share // sum(SHARES) for share in SHARES]

    def buffer(rows):
        return pltpu.VMEM((rows, channels), jnp.float32)

    one = pltpu.SemaphoreType.DMA
    few = pltpu.SemaphoreType.DMA((len(sizes),))
    sems = pltpu.SemaphoreType.DMA((2 * len(sizes),))
    out = pl.pallas_call(
        functools.partial(kernel, n, sizes),
        out_shape=buffer(steps),
        in_specs=[pl.BlockSpec(memory_space=pl.ANY)] * 2,
        out_specs=pl.BlockSpec(memory_space=pltpu.VMEM),
        scratch_shapes=[buffer(steps)] * 3
        + [buffer(steps // 2), buffer(tap_gain.shape[0]), one]
        + [sems, one, sems, one, sems]
        + [buffer(2 * sizes[DETOURS[0]]), pltpu.SemaphoreType.DMA((2,)), pltpu.SemaphoreType.DMA((2,))]
        + [buffer(steps // 2), one, few] * 2,
        compiler_params=pltpu.CompilerParams(
            collective_id=0, has_side_effects=True, vmem_limit_bytes=52 * 2**20
        ),
        name="echo",
    )(signal, tap_gain)
    return out.reshape(signal.shape)


def solution(mesh):
    in_specs = (P("track", "lane", None, None), P())
    out_specs = P("track", "lane", None, None)
    body = functools.partial(local, mesh.shape["track"])
    return jax.shard_map(body, mesh=mesh, in_specs=in_specs, out_specs=out_specs, check_vma=False)
```
